512 devices in a mesh: grp: 2 (over y), tp: 128 (over x, z), sub: 2 (over core).
Axes of the slice: x: 8, y: 2, z: 16, core: 2. Of those that a mesh axis runs over, the one named last changes fastest.
The devices are a block of a 8x8x16 slice.
Arguments:
- hidden_in: bfloat16 [32, 2, 4096], P('grp', 'sub', 'tp'), parts along dimension 0, may hold values from -16 to 16
- norm_attn: float32 [8192], replicated, may hold values from 0.25 to 1.75
- w_query: bfloat16 [8192, 2, 4096], P(None, 'sub', 'tp'), may hold values from -0.0625 to 0.0625
- w_key: bfloat16 [8192, 2, 512], P(None, 'sub', 'tp'), may hold values from -0.0625 to 0.0625
- w_value: bfloat16 [8192, 2, 512], P(None, 'sub', 'tp'), may hold values from -0.0625 to 0.0625
- w_out: bfloat16 [2, 4096, 2, 4096], P('sub', None, None, 'tp'), may hold values from -0.0625 to 0.0625
- norm_ffn: float32 [8192], replicated, may hold values from 0.25 to 1.75
- w_gate: bfloat16 [2, 4096, 14336], P('sub', None, 'tp'), may hold values from -0.0625 to 0.0625
- w_up: bfloat16 [2, 4096, 14336], P('sub', None, 'tp'), may hold values from -0.0625 to 0.0625
- w_down: bfloat16 [14336, 2, 4096], P('tp', 'sub'), may hold values from -0.1875 to 0.1875
- cache_keys: bfloat16 [32, 1024, 8, 128], P('grp', 'tp', 'sub'), parts along dimension 0, may hold values from -250 to 250
- cache_values: bfloat16 [32, 1024, 8, 128], P('grp', 'tp', 'sub'), parts along dimension 0, may hold values from -6 to 6
- lengths: int32 [32], P('grp'), parts along dimension 0, may hold values from 1 to 1024, as said below
Outputs:
- hidden_out: bfloat16 [32, 2, 4096], P('grp', 'sub', 'tp'), parts along dimension 0
The draws below stay inside these ranges and needn't reach their ends.
There are 2 independent parts, one for each index of `grp`. The reference program is written for one: setup_inputs(seed, part) draws one part's arguments, and reference() takes and returns one part's arrays. A program takes and returns all parts, laid end to end along the dimension named above; an argument that names none is the same for every part. Nothing has to cross between parts.
Inputs may be any that keep to these rules, and one draw needn't show every extreme that they name: `lengths`: some sequence has 1024 live positions and some has 1.
All inputs are finite; a program needn't handle non-finite values.
Results may differ from the reference program's by a relative error of at most 0.012.
The reference program's roundings to bfloat16 on the way (of `normed`, `attended`, `middle`, `normed_ffn` and `hidden`) count: a program that leaves them out, or rounds other values in their place, can miss the bound.
Values may be sent and summed in bfloat16 or wider, within the bound.
A program may use at most 128 MiB of HBM per device.

```python
import math
import jax
import jax.numpy as jnp
from jax import lax

D = 8192
HQ = 64
HK = 8
HD = 128
FF = 14336
SEQS = 16
CACHE_LEN = 1024
N_SUB = 2


def draw_hidden_in(key, part):
    base_key = jax.random.fold_in(key, 101)
    key_noise, key_rows, key_cols = jax.random.split(base_key, 3)
    ramp = jnp.sqrt(1.0 + 2.0 * jnp.arange(D, dtype=jnp.float32) / (D - 1))
    noise = jnp.clip(jax.random.normal(key_noise, (SEQS, D), jnp.float32), -4.0, 4.0)
    row_scale = jnp.exp(jax.random.uniform(key_rows, (SEQS, 1), jnp.float32, math.log(0.5), math.log(2.0)))
    column_scale = jnp.exp(jax.random.uniform(key_cols, (1, D), jnp.float32, math.log(0.5), math.log(2.0)))
    values = jnp.clip(noise * row_scale * column_scale * ramp[None, :], -16.0, 16.0)
    return values.reshape(SEQS, N_SUB, D // N_SUB).astype(jnp.bfloat16)


def draw_cache_keys(key, part):
    base_key = jax.random.fold_in(key, 202)
    key_noise, key_pick, key_strength = jax.random.split(base_key, 3)
    noise = jnp.clip(jax.random.normal(key_noise, (SEQS, CACHE_LEN, HK, HD), jnp.float32), -2.0, 2.0)
    strength = jnp.exp(jax.random.uniform(key_strength, (SEQS, CACHE_LEN), jnp.float32, math.log(40.0), math.log(120.0)))
    picked = jax.random.uniform(key_pick, (SEQS, CACHE_LEN), jnp.float32) < 0.1
    boosted = noise * jnp.where(picked, strength, 1.0)[:, :, None, None]
    twins = jnp.concatenate([boosted[:, :1], boosted[:, :-1] * 1.01], axis=1)
    follows = jnp.concatenate([jnp.zeros((SEQS, 1), dtype=bool), picked[:, :-1]], axis=1)
    values = jnp.where(follows[:, :, None, None], twins, boosted)
    return jnp.clip(values, -250.0, 250.0).astype(jnp.bfloat16)


def draw_lengths(key, part):
    base_key = jax.random.fold_in(key, 303)
    key_values, key_order = jax.random.split(base_key, 2)
    values = jax.random.randint(key_values, (SEQS,), 1, CACHE_LEN + 1, dtype=jnp.int32)
    order = jax.random.permutation(key_order, SEQS)
    values = values.at[order[0]].set(CACHE_LEN)
    values = values.at[order[1]].set(1)
    return values.astype(jnp.int32)


def raised(values, key, source, target, blocks, factor):
    owner, partner = [(jnp.arange(values.shape[position]) // (values.shape[position] // blocks)).reshape([-1 if axis == position else 1 for axis in range(values.ndim)]) for position in (source, target)]
    chosen = jax.random.permutation(key, blocks)[partner]
    strong = (owner == chosen) | (owner == (partner + blocks // 2) % blocks)
    return jnp.where(strong, factor * values, values)


def block_scale(own_key, dims, pieces, smallest, top_value):
    def one(dim, shards_of):
        heights = jax.random.uniform(jax.random.fold_in(jax.random.fold_in(own_key, 6), dim), (shards_of,), jnp.float32, smallest / len(pieces), top_value / len(pieces))
        return jnp.repeat(jnp.exp(heights), dims[dim] // shards_of).reshape((-1,) + (1,) * (len(dims) - dim - 1))

    factor_of = one(*pieces[0])
    for cut in pieces[1:]:
        factor_of = factor_of * one(*cut)
    return factor_of


def normal_values(rng, extent, spread, limit, cuts=(), kind=jnp.bfloat16):
    array = spread * jax.random.normal(rng, extent, jnp.float32)
    if cuts:
        array = array * block_scale(rng, extent, cuts, -0.22, 0.18)
    return jnp.clip(array, -limit, limit).astype(kind)


def bell_draw_with(key, dims, deviation, bound, pieces, heavy, held_as=jnp.bfloat16):
    array = deviation * jax.random.normal(key, dims, jnp.float32)
    if pieces:
        array = array * block_scale(key, dims, pieces, -0.22, 0.18)
    return jnp.clip(raised(array, jax.random.fold_in(key, 3), *heavy), -bound, bound).astype(held_as)


def setup_inputs(seed: int = 0, part: int = 0) -> dict:
    arg_keys = jax.random.split(jax.random.key(seed), 14)
    part_splits = jax.random.split(jax.random.fold_in(arg_keys[13], part), 14)
    hidden_in = draw_hidden_in(jax.random.fold_in(jax.random.fold_in(arg_keys[13], part), 71), part)
    norm_attn = jnp.clip(1.0 + 0.15 * jax.random.normal(arg_keys[1], (D,), jnp.float32), 0.25, 1.75)
    w_query = normal_values(arg_keys[2], (D, N_SUB, HQ * HD // N_SUB), D ** -0.5, 0.0625, ((1, 2), (2, 128)))
    w_key = normal_values(arg_keys[3], (D, N_SUB, HK * HD // N_SUB), D ** -0.5, 0.0625, ((1, 2), (2, 128)))
    w_value = normal_values(arg_keys[4], (D, N_SUB, HK * HD // N_SUB), D ** -0.5, 0.0625, ((1, 2), (2, 128)))
    w_out = normal_values(arg_keys[5], (N_SUB, HQ * HD // N_SUB, N_SUB, D // N_SUB), (HQ * HD) ** -0.5, 0.0625, ((0, 2), (3, 128)))
    norm_ffn = jnp.clip(1.0 + 0.15 * jax.random.normal(arg_keys[6], (D,), jnp.float32), 0.25, 1.75)
    w_gate = normal_values(arg_keys[7], (N_SUB, D // N_SUB, FF), D ** -0.5, 0.0625, ((0, 2), (2, 128)))
    w_up = normal_values(arg_keys[8], (N_SUB, D // N_SUB, FF), D ** -0.5, 0.0625, ((0, 2), (2, 128)))
    w_down = bell_draw_with(arg_keys[9], (FF, N_SUB, D // N_SUB), FF ** -0.5, 0.1875, ((0, 128), (1, 2)), (0, 2, 128, 5.5))
    cache_keys = draw_cache_keys(jax.random.fold_in(jax.random.fold_in(arg_keys[13], part), 71), part)
    cache_values = normal_values(part_splits[11], (SEQS, CACHE_LEN, HK, HD), 1.0, 6.0, ((1, 128), (2, 2)))
    lengths = draw_lengths(jax.random.fold_in(jax.random.fold_in(arg_keys[13], part), 71), part)
    return {"hidden_in": hidden_in, "norm_attn": norm_attn, "w_query": w_query, "w_key": w_key, "w_value": w_value, "w_out": w_out, "norm_ffn": norm_ffn, "w_gate": w_gate, "w_up": w_up, "w_down": w_down, "cache_keys": cache_keys, "cache_values": cache_values, "lengths": lengths}


epsilon = 1e-05
rope_base = 500000.0
floor_score = -1e+30

def rms_norm(values, gain):
    mean_square = lax.optimization_barrier(jnp.mean(values * values, axis=-1, keepdims=True))
    return (values * lax.rsqrt(mean_square + epsilon) * gain.astype(jnp.float32)).astype(jnp.bfloat16)

def rope_angles(lengths):
    frequencies = rope_base ** (-(jnp.arange(HD // 2, dtype=jnp.float32) * 2.0) / HD)
    return lengths.astype(jnp.float32)[:, None] * frequencies[None, :]

def rotate(vectors, angles):
    middle_index = vectors.shape[-1] // 2
    cosine = jnp.cos(angles)[:, None, :]
    sine = jnp.sin(angles)[:, None, :]
    lower = vectors[..., :middle_index]
    upper = vectors[..., middle_index:]
    return jnp.concatenate([lower * cosine - upper * sine, upper * cosine + lower * sine], axis=-1)

def reference(hidden_in, norm_attn, w_query, w_key, w_value, w_out, norm_ffn, w_gate, w_up, w_down, cache_keys, cache_values, lengths):
    residual = hidden_in.reshape(SEQS, D).astype(jnp.float32)
    normed = rms_norm(residual, norm_attn)
    query = jnp.dot(normed, w_query.reshape(D, HQ * HD), preferred_element_type=jnp.float32).astype(jnp.bfloat16)
    key_new = jnp.dot(normed, w_key.reshape(D, HK * HD), preferred_element_type=jnp.float32).astype(jnp.bfloat16)
    value_new = jnp.dot(normed, w_value.reshape(D, HK * HD), preferred_element_type=jnp.float32).astype(jnp.bfloat16)
    angles = rope_angles(lengths)
    query_rot = rotate(query.astype(jnp.float32).reshape(SEQS, HQ, HD), angles).astype(jnp.bfloat16)
    key_rot = rotate(key_new.astype(jnp.float32).reshape(SEQS, HK, HD), angles).astype(jnp.bfloat16)
    group_size = HQ // HK
    grouped = query_rot.astype(jnp.float32).reshape(SEQS, HK, group_size, HD)
    scores = jnp.einsum('bkgd,blkd->bkgl', grouped, cache_keys.astype(jnp.float32), precision=lax.Precision.HIGHEST) / math.sqrt(HD)
    places = jnp.arange(cache_keys.shape[1], dtype=jnp.int32)
    live = (places[None, :] < lengths[:, None])[:, None, None, :]
    masked = jnp.where(live, scores, floor_score)
    own_score = lax.optimization_barrier(jnp.sum(grouped * key_rot.astype(jnp.float32)[:, :, None, :], axis=-1)) / math.sqrt(HD)
    highest = jnp.maximum(lax.optimization_barrier(jnp.max(masked, axis=-1)), own_score)
    weights = jnp.where(live, jnp.exp(masked - highest[..., None]), 0.0)
    own_weight = jnp.exp(own_score - highest)
    numerator = jnp.einsum('bkgl,blkd->bkgd', weights, cache_values.astype(jnp.float32), precision=lax.Precision.HIGHEST)
    numerator = numerator + own_weight[..., None] * value_new.astype(jnp.float32).reshape(SEQS, HK, 1, HD)
    denominator = lax.optimization_barrier(jnp.sum(weights, axis=-1)) + own_weight
    attended = (numerator / denominator[..., None]).reshape(SEQS, HQ * HD).astype(jnp.bfloat16)
    mixed = jnp.dot(attended, w_out.reshape(HQ * HD, D), preferred_element_type=jnp.float32)
    middle = (residual + mixed).astype(jnp.bfloat16)
    normed_ffn = rms_norm(middle.astype(jnp.float32), norm_ffn)
    gate = jnp.dot(normed_ffn, w_gate.reshape(D, FF), preferred_element_type=jnp.float32)
    up_value = jnp.dot(normed_ffn, w_up.reshape(D, FF), preferred_element_type=jnp.float32)
    hidden = (jax.nn.silu(gate) * up_value).astype(jnp.bfloat16)
    down_value = jnp.dot(hidden, w_down.reshape(FF, D), preferred_element_type=jnp.float32)
    result = (middle.astype(jnp.float32) + down_value).astype(jnp.bfloat16)
    return result.reshape(SEQS, N_SUB, D // N_SUB)
```

```python
import math

import jax
import jax.numpy as jnp
import numpy as np
from jax import lax
from jax.experimental import pallas as pl
from jax.experimental.pallas import tpu as pltpu
from jax.sharding import PartitionSpec as P

HD = 128
NX, NZ = 8, 16
MESH = pl.DeviceIdType.MESH
EPS = 1e-05
ROPE_BASE = 500000.0
FLOOR = -1e30
F32, BF16 = jnp.float32, jnp.bfloat16

Z_ORDER = [8, 7, 9, 6, 10, 5, 11, 4, 12, 3, 13, 2, 14, 1, 15]
X_ORDER = [4, 3, 5, 2, 6, 1, 7]
X_ARRIVAL = [1, 7, 2, 6, 3, 5, 4]


def nt_dot(a, b):
    return lax.dot_general(a, b, (((1,), (1,)), ((), ())), preferred_element_type=F32)


def iota(shape, dim):
    return lax.broadcasted_iota(jnp.int32, shape, dim)


def block_transpose(t):
    turn = (iota(t.shape, 0) // 4 - iota(t.shape, 1) // 32 + 4) % 4
    out = t
    for d in range(1, 4):
        moved = pltpu.roll(pltpu.roll(t, 128 - 32 * d, axis=1), 4 * d, axis=0)
        out = jnp.where(turn == d, moved, out)
    return out


def widened(v, lanes=128):
    return jnp.concatenate([v, jnp.zeros((v.shape[0], lanes - v.shape[1]), v.dtype)], axis=1)


def cos_sin(angle):
    turns = jnp.floor(angle * (2.0 / math.pi) + 0.5)
    r = angle - turns * 1.5703125
    r = r - turns * 4.837512969970703125e-4
    r = r - turns * 7.54978995489188216e-8
    r2 = r * r
    sine = r + r * r2 * (-1.6666654611e-1 + r2 * (8.3321608736e-3 + r2 * -1.9515295891e-4))
    cosine = 1.0 - 0.5 * r2 + r2 * r2 * (
        4.166664568298827e-2 + r2 * (-1.388731625493765e-3 + r2 * 2.443315711809948e-5)
    )
    quarter = turns.astype(jnp.int32) & 3
    odd = (quarter & 1) == 1
    c = jnp.where(odd, sine, cosine)
    s = jnp.where(odd, cosine, sine)
    c = jnp.where((quarter == 1) | (quarter == 2), -c, c)
    s = jnp.where(quarter >= 2, -s, s)
    return c, s


def kernel(
    hid, gain_a, wq, wk, wv, wo, gain_f, wg, wu, wd, ck, cv, lens, freq,
    out,
    hid_v, ga_v, gf_v, wcat, wk_v, wv_v, wo_v, wg_v, wu_v, wd_v, kb, vb, kx, vx, len_v, freq_v,
    h1s, h1r, xall, qs, qr, qxs, qxr, ps, pr, ats, atr, axs, axr, mos, mor,
    mzs, mzr, mxs, mxr, ges, ger, dxs, dxr, dzs, dzr,
    local, ssem, rsem, xr_hid, xr_att, xr_mid, fwd_r,
):
    g, tp, s = lax.axis_index("grp"), lax.axis_index("tp"), lax.axis_index("sub")
    x, z = tp // NZ, tp % NZ
    seqs = hid_v.shape[0]
    half = wo_v.shape[1]
    block = half // NX

    def z_peer(o):
        return (z + o) % NZ

    def x_peer(o):
        return (x + o) % NX

    def at(px, pz):
        return (g, px * NZ + pz, s)

    partner = (g, tp, 1 - s)

    barrier = pltpu.get_barrier_semaphore()
    for o in Z_ORDER:
        pl.semaphore_signal(barrier, 1, device_id=at(x, z_peer(o)), device_id_type=MESH)
    for o in X_ORDER:
        pl.semaphore_signal(barrier, 1, device_id=at(x_peer(o), z), device_id_type=MESH)
    pl.semaphore_signal(barrier, 1, device_id=partner, device_id_type=MESH)

    def fetch(k, src, dst):
        copy = pltpu.make_async_copy(src, dst, local.at[k])
        copy.start()
        return copy

    got_hid = fetch(0, hid, hid_v)
    rows_q = wq.shape[0]
    span = ck.shape[1]
    got_first = [
        fetch(1, lens, len_v),
        fetch(2, freq, freq_v),
        fetch(3, wk, wk_v),
        fetch(4, wv, wv_v),
        fetch(5, wq, wcat.at[pl.ds(0, rows_q)]),
        fetch(6, gain_a, ga_v),
    ]
    got_cache = [
        fetch(7, ck.at[z], kb.at[z]),
        fetch(8, cv.at[z], vb.at[z]),
    ]
    got_later = [
        fetch(9, wo, wo_v),
        fetch(10, gain_f.at[:, pl.ds(pl.multiple_of(s * half, half), half)], gf_v),
        fetch(11, wg, wg_v),
        fetch(12, wu, wu_v),
        fetch(13, wd, wd_v),
    ]

    def remote(src, dst, k, device, recv=None):
        return pltpu.make_async_remote_copy(
            src_ref=src,
            dst_ref=dst,
            send_sem=ssem.at[k],
            recv_sem=rsem.at[k] if recv is None else recv,
            device_id=device,
            device_id_type=MESH,
        )

    def z_send(k, src_of, dst):
        for o in Z_ORDER:
            p = z_peer(o)
            remote(src_of(p), dst.at[z], k, at(x, p)).start()

    def z_bytes(k, buf):
        part = buf.at[pl.ds(0, NZ - 1)]
        return remote(part, part, k, at(x, z_peer(1)))

    def x_send(k, src_of, dst, recv=None):
        for o in X_ORDER:
            p = x_peer(o)
            remote(
                src_of(p), dst.at[x], k, at(p, z), None if recv is None else recv.at[x]
            ).start()

    def x_bytes(k, buf):
        part = buf.at[pl.ds(0, NX - 1)]
        return remote(part, part, k, at(x_peer(1), z))

    def x_wait_one(k, buf, recv, p):
        remote(buf.at[p], buf.at[p], k, at(x_peer(1), z), recv.at[p]).wait_recv()

    def packed(v):
        return block_transpose(widened(v))[:4]

    def unpack_rows(buf, dst):
        for m in range(NZ // 4):
            tile = jnp.concatenate([buf[4 * m + i].astype(F32) for i in range(4)], axis=0)
            dst[:, 128 * m : 128 * m + 128] = block_transpose(tile).astype(BF16)

    got_hid.wait()
    residual = hid_v[...].astype(F32)
    first = packed(residual).astype(BF16)
    h1s[...] = first
    h1r[z] = first
    pl.semaphore_wait(barrier, NZ - 1 + NX - 1 + 1)
    z_send(0, lambda p: h1s, h1r)

    for c in got_first:
        c.wait()
    lanes = 1024
    for c in range(wcat.shape[1] // lanes):
        cols = pl.ds(c * lanes, lanes)
        both = jnp.concatenate([wk_v[:, cols].astype(F32), wv_v[:, cols].astype(F32)], axis=0)
        both = jnp.concatenate([both, jnp.zeros_like(both)], axis=0)
        wcat[rows_q : rows_q + 16, cols] = both.astype(BF16)
    lane1 = iota((1, 128), 1)
    mine = jnp.where(iota(len_v.shape, 1) == z, len_v[...], 0)
    length = jnp.sum(mine, axis=1, keepdims=True)
    cosine, sine = cos_sin(length.astype(F32) * freq_v[...])
    sine = jnp.where(lane1 < HD // 2, -sine, sine)

    z_bytes(0, h1r).wait_recv()
    own_block = xall.at[s, x]
    unpack_rows(h1r, own_block)
    x_send(1, lambda p: own_block, xall.at[s], xr_hid)

    z_send(2, lambda p: ck.at[p], kb)
    z_send(3, lambda p: cv.at[p], vb)

    def forward(p):
        return remote(xall.at[s, p], xall.at[s, p], 4, partner, fwd_r.at[p])

    squares = jnp.zeros((seqs, 128), F32)

    def fold(v):
        v = v * v
        total = v[:, :128]
        for c in range(1, v.shape[1] // 128):
            total = total + v[:, 128 * c : 128 * c + 128]
        return total

    forward(x).start()
    squares = squares + fold(own_block[...].astype(F32))
    for o in X_ARRIVAL:
        p = x_peer(o)
        x_wait_one(1, xall.at[s], xr_hid, p)
        forward(p).start()
        squares = squares + fold(xall[s, p].astype(F32))
    for o in [0] + X_ARRIVAL:
        p = x_peer(o)
        part = xall.at[1 - s, p]
        remote(part, part, 4, partner, fwd_r.at[p]).wait_recv()
        squares = squares + fold(xall[1 - s, p].astype(F32))
    factor = lax.rsqrt(jnp.sum(squares, axis=1, keepdims=True) / (2 * half) + EPS)

    qkv = jnp.zeros((seqs, wcat.shape[0]), F32)
    for h in range(2):
        for p in range(NX):
            cols = pl.ds(h * half + p * block, block)
            normed = (xall[h, p].astype(F32) * factor * ga_v[:, cols]).astype(BF16)
            qkv = qkv + nt_dot(normed, wcat[:, cols])
    qkv = widened(qkv.astype(BF16).astype(F32))
    per = wk_v.shape[0]
    lane = iota((seqs, 128), 1)
    q_row = pltpu.roll(jnp.where(lane < rows_q, qkv, 0.0), rows_q * (z % 4), axis=1)
    k_only = jnp.where((lane >= rows_q) & (lane < rows_q + per), qkv, 0.0)
    v_only = jnp.where((lane >= rows_q + per) & (lane < rows_q + 2 * per), qkv, 0.0)
    kv_row = pltpu.roll(k_only, (128 - rows_q + per * z) % 128, axis=1) + pltpu.roll(
        v_only, (128 - rows_q - per + 64 + per * z) % 128, axis=1
    )
    for b in range(seqs):
        qs[b] = jnp.concatenate([q_row[b : b + 1], kv_row[b : b + 1]], axis=0)
    qr[z] = qs[z]
    z_send(5, lambda p: qs.at[p], qr)
    z_bytes(5, qr).wait_recv()
    heads = [qr[4 * h] + qr[4 * h + 1] + qr[4 * h + 2] + qr[4 * h + 3] for h in range(NZ // 4)]
    kv_sum = heads[0] + heads[1] + heads[2] + heads[3]
    rows = [h[0:1] for h in heads] + [kv_sum[1:2], jnp.zeros((3, 128), F32)]
    message = jnp.concatenate(rows, axis=0).astype(BF16)
    qxs[...] = message
    qxr[x] = message
    x_send(6, lambda p: qxs, qxr)
    x_bytes(6, qxr).wait_recv()

    arrived = [qxr[p].astype(F32) for p in range(NX)]
    kv_rows = [a[4:5] for a in arrived]
    low = lane1 < 64
    new_keys, new_values = [], []
    for k in range(NX // 2):
        a, b = kv_rows[2 * k], kv_rows[2 * k + 1]
        new_keys.append(jnp.where(low, a, pltpu.roll(b, 64, axis=1)))
        new_values.append(jnp.where(low, pltpu.roll(a, 64, axis=1), b))
    nk = len(new_keys)

    def rotated(v):
        return (v * cosine + pltpu.roll(v, HD // 2, axis=1) * sine).astype(BF16)

    query = rotated(jnp.concatenate([a[0:4] for a in arrived], axis=0))
    fill = jnp.zeros((16 - nk, 128), F32)
    kx[...] = rotated(jnp.concatenate(new_keys + [fill], axis=0))
    vx[...] = jnp.concatenate(new_values + [fill], axis=0).astype(BF16)

    for c in got_cache:
        c.wait()
    z_bytes(2, kb).wait_recv()
    n_heads = query.shape[0]
    group = n_heads // nk
    keys = kb[...].reshape(NZ * span, HD)
    cached = nt_dot(query, keys) * (1.0 / math.sqrt(HD))
    own = nt_dot(query, kx[...]) * (1.0 / math.sqrt(HD))
    n_cached = NZ * span
    row_c, lane_c = iota(cached.shape, 0), iota(cached.shape, 1)
    place = x * (n_cached // nk) + lane_c // nk
    live_c = (place < length) & (lane_c % nk == row_c // group)
    row_o, lane_o = iota(own.shape, 0), iota(own.shape, 1)
    live_o = (lane_o == row_o // group) & (x == 0)
    cached = jnp.where(live_c, cached, FLOOR)
    own = jnp.where(live_o, own, FLOOR)
    top = jnp.maximum(
        jnp.max(cached, axis=1, keepdims=True), jnp.max(own, axis=1, keepdims=True)
    )
    w_c = jnp.where(live_c, jnp.exp(cached - top), 0.0)
    w_o = jnp.where(live_o, jnp.exp(own - top), 0.0)
    total = jnp.sum(w_c, axis=1, keepdims=True) + jnp.sum(w_o, axis=1, keepdims=True)
    z_bytes(3, vb).wait_recv()
    values = vb[...].reshape(NZ * span, HD)

    def weighted(w, v):
        high = w.astype(BF16)
        rest = (w - high.astype(F32)).astype(BF16)
        return jnp.dot(high, v, preferred_element_type=F32) + jnp.dot(
            rest, v, preferred_element_type=F32
        )

    mixed = weighted(w_c, values) + weighted(w_o, vx[...])
    lane_h = iota((n_heads, 128), 1)
    stats = jnp.where(lane_h < 64, top, total)
    for p in range(NX):
        ps[p] = jnp.concatenate([mixed[4 * p : 4 * p + 4], stats[4 * p : 4 * p + 4]], axis=0)
    pr[x] = ps[x]
    x_send(7, lambda p: ps.at[p], pr)
    x_bytes(7, pr).wait_recv()
    parts = [pr[p] for p in range(NX)]
    lane4 = iota((4, 128), 1)
    tops, sums = [], []
    for part in parts:
        st = part[4:8]
        turned = pltpu.roll(st, 64, axis=1)
        tops.append(jnp.where(lane4 < 64, st, turned))
        sums.append(jnp.where(lane4 < 64, turned, st))
    highest = tops[0]
    for t in tops[1:]:
        highest = jnp.maximum(highest, t)
    numerator = jnp.zeros((4, 128), F32)
    denominator = jnp.zeros((4, 128), F32)
    for part, t, l in zip(parts, tops, sums):
        scale = jnp.exp(t - highest)
        numerator = numerator + part[0:4] * scale
        denominator = denominator + l * scale
    attended = (numerator / denominator).astype(BF16)
    ats[...] = attended
    atr[z] = attended
    z_send(8, lambda p: ats, atr)
    for c in got_later:
        c.wait()
    z_bytes(8, atr).wait_recv()
    rows4 = [atr[b].astype(F32) for b in range(seqs)]
    for h in range(4):
        axs[:, 128 * h : 128 * h + 128] = jnp.concatenate(
            [r[h : h + 1] for r in rows4], axis=0
        ).astype(BF16)
    x_send(9, lambda p: axs, axr, xr_att)

    def columns(p):
        return pl.ds(pl.multiple_of(p * block, block), block)

    out_part = nt_dot(axs[...], wo_v[:, columns(x)])
    for o in X_ARRIVAL:
        p = x_peer(o)
        x_wait_one(9, axr, xr_att, p)
        out_part = out_part + nt_dot(axr[p], wo_v[:, columns(p)])
    out_part = widened(out_part)
    mos[...] = out_part
    swap = remote(mos, mor, 10, partner)
    swap.start()
    swap.wait_recv()
    both = out_part + mor[...]
    width = hid_v.shape[1]
    both = jnp.where(s == 0, both, pltpu.roll(both, 128 - width, axis=1))
    middle = (residual + both[:, :width]).astype(BF16).astype(F32)

    first = packed(middle).astype(BF16)
    mzs[...] = first
    mzr[z] = first
    z_send(11, lambda p: mzs, mzr)
    z_bytes(11, mzr).wait_recv()
    unpack_rows(mzr, mxs)
    x_send(12, lambda p: mxs, mxr, xr_mid)
    units = wg_v.shape[0]
    gate = jnp.zeros((seqs, units), F32)
    up = jnp.zeros((seqs, units), F32)
    squares = jnp.zeros((seqs, 128), F32)
    for o in [0] + X_ARRIVAL:
        p = x_peer(o)
        if o:
            x_wait_one(12, mxr, xr_mid, p)
            piece = mxr[p].astype(F32)
        else:
            piece = mxs[...].astype(F32)
        squares = squares + fold(piece)
        scaled = (piece * gf_v[:, columns(p)]).astype(BF16)
        gate = gate + nt_dot(scaled, wg_v[:, columns(p)])
        up = up + nt_dot(scaled, wu_v[:, columns(p)])
    ges[0] = widened(gate)
    ges[1] = widened(up)
    ges[2] = squares
    swap2 = remote(ges, ger, 13, partner)
    swap2.start()
    swap2.wait_recv()
    squares = jnp.sum(squares + ger[2], axis=1, keepdims=True)
    factor = lax.rsqrt(squares / (2 * half) + EPS)
    gate = (gate + ger[0][:, :units]) * factor
    up = (up + ger[1][:, :units]) * factor
    hidden = (gate / (1.0 + jnp.exp(-gate)) * up).astype(BF16)
    for o in X_ORDER + [0]:
        p = x_peer(o)
        piece = jnp.dot(hidden, wd_v[:, columns(p)], preferred_element_type=F32).astype(BF16)
        if o:
            dxs[p] = piece
            remote(dxs.at[p], dxr.at[x], 14, at(p, z)).start()
        else:
            dxr[p] = piece
    x_bytes(14, dxr).wait_recv()
    total = dxr[0].astype(F32)
    for p in range(1, NX):
        total = total + dxr[p].astype(F32)
    for m in range(NZ // 4):
        tile = block_transpose(total[:, 128 * m : 128 * m + 128])
        for i in range(4):
            dzs[4 * m + i] = tile[4 * i : 4 * i + 4].astype(BF16)
    dzr[z] = dzs[z]
    z_send(15, lambda p: dzs.at[p], dzr)
    z_bytes(15, dzr).wait_recv()
    total = dzr[0].astype(F32)
    for p in range(1, NZ):
        total = total + dzr[p].astype(F32)
    total = jnp.concatenate([total, jnp.zeros((12, 128), F32)], axis=0)
    down = block_transpose(total)[:, :width]
    out[...] = (middle + down).astype(BF16)

    z_bytes(0, h1r).wait_send()
    x_bytes(1, xall.at[s]).wait_send()
    z_bytes(2, kb).wait_send()
    z_bytes(3, vb).wait_send()
    remote(xall.at[s], xall.at[s], 4, partner).wait_send()
    z_bytes(5, qr).wait_send()
    x_bytes(6, qxr).wait_send()
    x_bytes(7, pr).wait_send()
    z_bytes(8, atr).wait_send()
    x_bytes(9, axr).wait_send()
    swap.wait_send()
    z_bytes(11, mzr).wait_send()
    x_bytes(12, mxr).wait_send()
    swap2.wait_send()
    x_bytes(14, dxr).wait_send()
    z_bytes(15, dzr).wait_send()


def per_device(
    hidden_in, norm_attn, w_query, w_key, w_value, w_out, norm_ffn,
    w_gate, w_up, w_down, cache_keys, cache_values, lengths,
):
    seqs, _, width = hidden_in.shape
    model = w_query.shape[0]
    half = w_gate.shape[1]
    block = half // NX
    units = w_gate.shape[2]
    rows_q, rows_k = w_query.shape[2], w_key.shape[2]
    span, nk = cache_keys.shape[1], cache_keys.shape[2]
    freq = ROPE_BASE ** (-(np.arange(HD // 2, dtype=np.float64) * 2.0) / HD)
    freq = jnp.asarray(np.concatenate([freq, freq])[None].astype(np.float32))
    operands = (
        hidden_in.reshape(seqs, width),
        norm_attn.reshape(1, model),
        w_query.reshape(model, rows_q).T,
        w_key.reshape(model, rows_k).T,
        w_value.reshape(model, rows_k).T,
        w_out.reshape(half, -1).T,
        norm_ffn.reshape(1, model),
        w_gate.reshape(half, units).T,
        w_up.reshape(half, units).T,
        w_down.reshape(units, half),
        cache_keys.reshape(seqs, span * nk, HD),
        cache_values.reshape(seqs, span * nk, HD),
        lengths.reshape(1, seqs),
        freq,
    )
    vm = pltpu.VMEM
    scratch = [
        vm((seqs, width), BF16),
        vm((1, model), F32),
        vm((1, half), F32),
        vm((rows_q + 16, model), BF16),
        vm((rows_k, model), BF16),
        vm((rows_k, model), BF16),
        vm((operands[5].shape[0], half), BF16),
        vm((units, half), BF16),
        vm((units, half), BF16),
        vm((units, half), BF16),
        vm((NZ, span * nk, HD), BF16),
        vm((NZ, span * nk, HD), BF16),
        vm((16, HD), BF16),
        vm((16, HD), BF16),
        vm((1, seqs), jnp.int32),
        vm((1, 128), F32),
        vm((4, 128), BF16),
        vm((NZ, 4, 128), BF16),
        vm((2, NX, seqs, block), BF16),
        vm((seqs, 2, 128), F32),
        vm((NZ, 2, 128), F32),
        vm((8, 128), BF16),
        vm((NX, 8, 128), BF16),
        vm((NX, 8, 128), F32),
        vm((NX, 8, 128), F32),
        vm((4, 128), BF16),
        vm((NZ, 4, 128), BF16),
        vm((seqs, block), BF16),
        vm((NX, seqs, block), BF16),
        vm((seqs, 128), F32),
        vm((seqs, 128), F32),
        vm((4, 128), BF16),
        vm((NZ, 4, 128), BF16),
        vm((seqs, block), BF16),
        vm((NX, seqs, block), BF16),
        vm((3, seqs, 128), F32),
        vm((3, seqs, 128), F32),
        vm((NX, seqs, block), BF16),
        vm((NX, seqs, block), BF16),
        vm((NZ, 4, 128), BF16),
        vm((NZ, 4, 128), BF16),
        pltpu.SemaphoreType.DMA((14,)),
        pltpu.SemaphoreType.DMA((16,)),
        pltpu.SemaphoreType.DMA((16,)),
        pltpu.SemaphoreType.DMA((NX,)),
        pltpu.SemaphoreType.DMA((NX,)),
        pltpu.SemaphoreType.DMA((NX,)),
        pltpu.SemaphoreType.DMA((NX,)),
    ]
    result = pl.pallas_call(
        kernel,
        out_shape=jax.ShapeDtypeStruct((seqs, width), BF16),
        in_specs=[pl.BlockSpec(memory_space=pl.ANY)] * len(operands),
        out_specs=pl.BlockSpec(memory_space=pltpu.VMEM),
        scratch_shapes=scratch,
        compiler_params=pltpu.CompilerParams(
            collective_id=0, has_side_effects=True, vmem_limit_bytes=60 * 1024 * 1024
        ),
    )(*operands)
    return result.reshape(seqs, 1, width)


def solution(mesh):
    return jax.shard_map(
        per_device,
        mesh=mesh,
        in_specs=(
            P("grp", "sub", "tp"),
            P(),
            P(None, "sub", "tp"),
            P(None, "sub", "tp"),
            P(None, "sub", "tp"),
            P("sub", None, None, "tp"),
            P(),
            P("sub", None, "tp"),
            P("sub", None, "tp"),
            P("tp", "sub", None),
            P("grp", "tp", "sub", None),
            P("grp", "tp", "sub", None),
            P("grp"),
        ),
        out_specs=P("grp", "sub", "tp"),
        check_vma=False,
    )
```

```python
import math

import jax
import jax.numpy as jnp
import numpy as np
from jax import lax
from jax.experimental import pallas as pl
from jax.experimental.pallas import tpu as pltpu
from jax.sharding import PartitionSpec as P

HD = 128
NX, NZ = 8, 16
MESH = pl.DeviceIdType.MESH
EPS = 1e-05
ROPE_BASE = 500000.0
FLOOR = -1e30
F32, BF16 = jnp.float32, jnp.bfloat16

Z_ORDER = [8, 7, 9, 6, 10, 5, 11, 4, 12, 3, 13, 2, 14, 1, 15]
X_ORDER = [4, 3, 5, 2, 6, 1, 7]
X_ARRIVAL = [1, 7, 2, 6, 3, 5, 4]


def nt_dot(a, b):
    return lax.dot_general(a, b, (((1,), (1,)), ((), ())), preferred_element_type=F32)


def iota(shape, dim):
    return lax.broadcasted_iota(jnp.int32, shape, dim)


def block_transpose(t):
    turn = (iota(t.shape, 0) // 4 - iota(t.shape, 1) // 32 + 4) % 4
    out = t
    for d in range(1, 4):
        moved = pltpu.roll(pltpu.roll(t, 128 - 32 * d, axis=1), 4 * d, axis=0)
        out = jnp.where(turn == d, moved, out)
    return out


def widened(v, lanes=128):
    return jnp.concatenate([v, jnp.zeros((v.shape[0], lanes - v.shape[1]), v.dtype)], axis=1)


def cos_sin(angle):
    turns = jnp.floor(angle * (2.0 / math.pi) + 0.5)
    r = angle - turns * 1.5703125
    r = r - turns * 4.837512969970703125e-4
    r = r - turns * 7.54978995489188216e-8
    r2 = r * r
    sine = r + r * r2 * (-1.6666654611e-1 + r2 * (8.3321608736e-3 + r2 * -1.9515295891e-4))
    cosine = 1.0 - 0.5 * r2 + r2 * r2 * (
        4.166664568298827e-2 + r2 * (-1.388731625493765e-3 + r2 * 2.443315711809948e-5)
    )
    quarter = turns.astype(jnp.int32) & 3
    odd = (quarter & 1) == 1
    c = jnp.where(odd, sine, cosine)
    s = jnp.where(odd, cosine, sine)
    c = jnp.where((quarter == 1) | (quarter == 2), -c, c)
    s = jnp.where(quarter >= 2, -s, s)
    return c, s


def kernel(
    hid, gain_a, wq, wk, wv, wo, gain_f, wg, wu, wd, ck, cv, lens, freq,
    out,
    hid_v, ga_v, gf_v, wcat, wk_v, wv_v, wo_v, wg_v, wu_v, wd_v, kb, vb, kx, vx, len_v, freq_v,
    h1s, h1r, xall, qs, qr, qxs, qxr, ps, pr, ats, atr, axs, axr, mos, mor,
    mzs, mzr, mxs, mxr, ges, ger, dxs, dxr, dzs, dzr,
    local, ssem, rsem, ready, ready_core, ready_row, heard, hz_r, xr_early, xr_hid, xr_att, xr_mid, fwd_r,
):
    g, tp, s = lax.axis_index("grp"), lax.axis_index("tp"), lax.axis_index("sub")
    x, z = tp // NZ, tp % NZ
    seqs = hid_v.shape[0]
    half = wo_v.shape[1]
    block = half // NX

    def z_peer(o):
        return (z + o) % NZ

    def x_peer(o):
        return (x + o) % NX

    def at(px, pz):
        return (g, px * NZ + pz, s)

    partner = (g, tp, 1 - s)

    turn = jnp.where((x == 0) & (s == 0), 1, 0)
    r = (z + NZ - turn) % NZ

    def ranked(k):
        return at(x, (k + turn) % NZ)

    got_hid = pltpu.make_async_copy(hid, hid_v, local.at[0])
    got_hid.start()
    barrier = pltpu.get_barrier_semaphore()
    base = z == 1

    @pl.when(s == 1)
    def _():
        pl.semaphore_signal(barrier, 1, device_id=partner, device_id_type=MESH)

    for j in range(1, NZ):

        @pl.when(r + j < NZ)
        def _():
            pl.semaphore_signal(barrier, 1, device_id=ranked(r + j), device_id_type=MESH)

    @pl.when(base)
    def _():
        for o in X_ORDER:
            pl.semaphore_signal(barrier, 1, device_id=at(x_peer(o), z), device_id_type=MESH)

    def fetch(k, src, dst):
        copy = pltpu.make_async_copy(src, dst, local.at[k])
        copy.start()
        return copy

    rows_q = wq.shape[0]
    span = ck.shape[1]
    got_first = [
        fetch(1, lens, len_v),
        fetch(2, freq, freq_v),
        fetch(3, wk, wk_v),
        fetch(4, wv, wv_v),
        fetch(5, wq, wcat.at[pl.ds(0, rows_q)]),
        fetch(6, gain_a, ga_v),
    ]
    got_cache = [
        fetch(7, ck.at[z], kb.at[z]),
        fetch(8, cv.at[z], vb.at[z]),
    ]
    got_later = [
        fetch(9, wo, wo_v),
        fetch(10, gain_f.at[:, pl.ds(pl.multiple_of(s * half, half), half)], gf_v),
        fetch(11, wg, wg_v),
        fetch(12, wu, wu_v),
        fetch(13, wd, wd_v),
    ]

    def remote(src, dst, k, device, recv=None):
        return pltpu.make_async_remote_copy(
            src_ref=src,
            dst_ref=dst,
            send_sem=ssem.at[k],
            recv_sem=rsem.at[k] if recv is None else recv,
            device_id=device,
            device_id_type=MESH,
        )

    def z_send(k, src_of, dst):
        for o in Z_ORDER:
            p = z_peer(o)
            remote(src_of(p), dst.at[z], k, at(x, p)).start()

    def z_bytes(k, buf):
        part = buf.at[pl.ds(0, NZ - 1)]
        return remote(part, part, k, at(x, z_peer(1)))

    def x_send(k, src_of, dst, recv=None):
        for o in X_ORDER:
            p = x_peer(o)
            remote(
                src_of(p), dst.at[x], k, at(p, z), None if recv is None else recv.at[x]
            ).start()

    def x_bytes(k, buf):
        part = buf.at[pl.ds(0, NX - 1)]
        return remote(part, part, k, at(x_peer(1), z))

    def x_wait_one(k, buf, recv, p):
        remote(buf.at[p], buf.at[p], k, at(x_peer(1), z), recv.at[p]).wait_recv()

    def packed(v):
        return block_transpose(widened(v))[:4]

    def unpacked(chunks):
        tile = jnp.concatenate([c.astype(F32) for c in chunks], axis=0)
        return block_transpose(tile).astype(BF16)

    def unpack_rows(buf, dst):
        for m in range(NZ // 4):
            dst[:, 128 * m : 128 * m + 128] = unpacked([buf[4 * m + i] for i in range(4)])

    here = r + (1 - s) + jnp.where(base, NX - 1, 0)

    @pl.when(here > 0)
    def _():
        pl.semaphore_wait(barrier, here)

    for j in range(1, NZ):

        @pl.when(j <= r)
        def _():
            pl.semaphore_signal(ready.at[r], 1, device_id=ranked(r - j), device_id_type=MESH)

    @pl.when(s == 0)
    def _():
        pl.semaphore_signal(ready_core, 1, device_id=partner, device_id_type=MESH)

    got_hid.wait()
    residual = hid_v[...].astype(F32)
    first = packed(residual).astype(BF16)
    h1s[...] = first
    h1r[r] = first

    def chunk(c, src, device):
        return remote(src, h1r.at[c], 0, device, hz_r.at[c])

    for j in range(NZ - 1, 0, -1):

        @pl.when(j <= r)
        def _():
            chunk(r, h1s, ranked(r - j)).start()

    @pl.when(r < NZ - 1)
    def _():
        pl.semaphore_wait(ready.at[r + 1], 1)
        chunk(r, h1s, ranked(r + 1)).start()

    def wait_chunk(c, carry):
        chunk(c, h1r.at[c], partner).wait_recv()
        return carry

    lax.fori_loop(0, r, wait_chunk, 0)

    @pl.when(r < NZ - 2)
    def _():
        pl.semaphore_wait(ready.at[r + 2], 1)

        def pass_on(c, carry):
            chunk(c, h1r.at[c], ranked(r + 2)).start()
            return carry

        lax.fori_loop(0, r + 1, pass_on, 0)

    def send_cache(k):
        b = (k + turn) % NZ
        remote(ck.at[b], kb.at[z], 2, ranked(k)).start()
        remote(cv.at[b], vb.at[z], 3, ranked(k)).start()

    for j in range(1, NZ):

        @pl.when(j <= r)
        def _():
            send_cache(r - j)

    for c in got_first:
        c.wait()
    lanes = 1024
    for c in range(wcat.shape[1] // lanes):
        cols = pl.ds(c * lanes, lanes)
        both = jnp.concatenate([wk_v[:, cols].astype(F32), wv_v[:, cols].astype(F32)], axis=0)
        both = jnp.concatenate([both, jnp.zeros_like(both)], axis=0)
        wcat[rows_q : rows_q + 16, cols] = both.astype(BF16)
    lane1 = iota((1, 128), 1)
    mine = jnp.where(iota(len_v.shape, 1) == z, len_v[...], 0)
    length = jnp.sum(mine, axis=1, keepdims=True)
    cosine, sine = cos_sin(length.astype(F32) * freq_v[...])
    sine = jnp.where(lane1 < HD // 2, -sine, sine)

    def tell_x_peers(pz):
        for o in X_ORDER:
            pl.semaphore_signal(heard.at[pz], 1, device_id=at(x_peer(o), z), device_id_type=MESH)

    def tell_row(pz):
        pl.semaphore_wait(heard.at[pz], NX - 1)
        pl.semaphore_signal(ready_row, 1, device_id=at(x, pz), device_id_type=MESH)

    @pl.when(base & (turn == 0))
    def _():
        tell_x_peers(0)

    def send_cache_up(ranks):
        for k in ranks:

            @pl.when(k > r)
            def _():
                @pl.when(k > r + 2)
                def _():
                    pl.semaphore_wait(ready.at[k], 1)

                send_cache(k)

                @pl.when(base)
                def _():
                    tell_x_peers((k + turn) % NZ)

                    @pl.when(k > r + 1)
                    def _():
                        tell_row(k + turn - 1)

    send_cache_up(range(1, NZ - 2))

    own_block = xall.at[s, x]
    split = block // 2
    early = 12 - turn
    lax.fori_loop(r + 1, early, wait_chunk, 0)

    def unpack_tile(m):
        to = (m + 3) % 4 * 128
        chunks = [h1r[(4 * m + i + NZ - turn) % NZ] for i in range(4)]
        own_block[:, to : to + 128] = unpacked(chunks)

    def half_block(ref, late):
        return ref.at[:, split * late : split * late + split]

    def x_half(late, recv):
        for o in X_ORDER:
            p = x_peer(o)
            part = half_block(own_block, late)
            remote(part, part, 1, at(p, z), recv.at[x]).start()

    def x_wait_half(late, recv, p):
        part = half_block(xall.at[s, p], late)
        remote(part, part, 1, at(x_peer(1), z), recv.at[p]).wait_recv()

    unpack_tile(1)
    unpack_tile(2)
    send_cache_up(range(NZ - 2, NZ))

    @pl.when(base)
    def _():
        @pl.when(turn == 0)
        def _():
            tell_row(NZ - 1)

        tell_row(0)

    @pl.when(jnp.logical_not(base))
    def _():
        pl.semaphore_wait(ready_row, 1)

    x_half(0, xr_early)
    lax.fori_loop(jnp.maximum(r + 1, early), NZ, wait_chunk, 0)
    unpack_tile(3)
    unpack_tile(0)
    x_half(1, xr_hid)

    def forward(p):
        return remote(xall.at[s, p], xall.at[s, p], 4, partner, fwd_r.at[p])

    squares = jnp.zeros((seqs, 128), F32)

    def fold(v):
        v = v * v
        total = v[:, :128]
        for c in range(1, v.shape[1] // 128):
            total = total + v[:, 128 * c : 128 * c + 128]
        return total

    @pl.when(s == 1)
    def _():
        pl.semaphore_wait(ready_core, 1)

    forward(x).start()
    squares = squares + fold(own_block[...].astype(F32))
    for o in X_ARRIVAL:
        p = x_peer(o)
        x_wait_half(0, xr_early, p)
        x_wait_half(1, xr_hid, p)
        forward(p).start()
        squares = squares + fold(xall[s, p].astype(F32))
    for o in [0] + X_ARRIVAL:
        p = x_peer(o)
        part = xall.at[1 - s, p]
        remote(part, part, 4, partner, fwd_r.at[p]).wait_recv()
        squares = squares + fold(xall[1 - s, p].astype(F32))
    factor = lax.rsqrt(jnp.sum(squares, axis=1, keepdims=True) / (2 * half) + EPS)

    qkv = jnp.zeros((seqs, wcat.shape[0]), F32)
    for h in range(2):
        for p in range(NX):
            cols = pl.ds(h * half + p * block, block)
            piece = xall[h, p].astype(F32)
            piece = jnp.concatenate([piece[:, block - 128 :], piece[:, : block - 128]], axis=1)
            normed = (piece * factor * ga_v[:, cols]).astype(BF16)
            qkv = qkv + nt_dot(normed, wcat[:, cols])
    qkv = widened(qkv.astype(BF16).astype(F32))
    per = wk_v.shape[0]
    lane = iota((seqs, 128), 1)
    q_row = pltpu.roll(jnp.where(lane < rows_q, qkv, 0.0), rows_q * (z % 4), axis=1)
    k_only = jnp.where((lane >= rows_q) & (lane < rows_q + per), qkv, 0.0)
    v_only = jnp.where((lane >= rows_q + per) & (lane < rows_q + 2 * per), qkv, 0.0)
    kv_row = pltpu.roll(k_only, (128 - rows_q + per * z) % 128, axis=1) + pltpu.roll(
        v_only, (128 - rows_q - per + 64 + per * z) % 128, axis=1
    )
    for b in range(seqs):
        qs[b] = jnp.concatenate([q_row[b : b + 1], kv_row[b : b + 1]], axis=0)
    qr[z] = qs[z]
    z_send(5, lambda p: qs.at[p], qr)
    z_bytes(5, qr).wait_recv()
    heads = [qr[4 * h] + qr[4 * h + 1] + qr[4 * h + 2] + qr[4 * h + 3] for h in range(NZ // 4)]
    kv_sum = heads[0] + heads[1] + heads[2] + heads[3]
    rows = [h[0:1] for h in heads] + [kv_sum[1:2], jnp.zeros((3, 128), F32)]
    message = jnp.concatenate(rows, axis=0).astype(BF16)
    qxs[...] = message
    qxr[x] = message
    x_send(6, lambda p: qxs, qxr)
    x_bytes(6, qxr).wait_recv()

    arrived = [qxr[p].astype(F32) for p in range(NX)]
    kv_rows = [a[4:5] for a in arrived]
    low = lane1 < 64
    new_keys, new_values = [], []
    for k in range(NX // 2):
        a, b = kv_rows[2 * k], kv_rows[2 * k + 1]
        new_keys.append(jnp.where(low, a, pltpu.roll(b, 64, axis=1)))
        new_values.append(jnp.where(low, pltpu.roll(a, 64, axis=1), b))
    nk = len(new_keys)

    def rotated(v):
        return (v * cosine + pltpu.roll(v, HD // 2, axis=1) * sine).astype(BF16)

    query = rotated(jnp.concatenate([a[0:4] for a in arrived], axis=0))
    fill = jnp.zeros((16 - nk, 128), F32)
    kx[...] = rotated(jnp.concatenate(new_keys + [fill], axis=0))
    vx[...] = jnp.concatenate(new_values + [fill], axis=0).astype(BF16)

    for c in got_cache:
        c.wait()
    z_bytes(2, kb).wait_recv()
    n_heads = query.shape[0]
    group = n_heads // nk
    keys = kb[...].reshape(NZ * span, HD)
    cached = nt_dot(query, keys) * (1.0 / math.sqrt(HD))
    own = nt_dot(query, kx[...]) * (1.0 / math.sqrt(HD))
    n_cached = NZ * span
    row_c, lane_c = iota(cached.shape, 0), iota(cached.shape, 1)
    place = x * (n_cached // nk) + lane_c // nk
    live_c = (place < length) & (lane_c % nk == row_c // group)
    row_o, lane_o = iota(own.shape, 0), iota(own.shape, 1)
    live_o = (lane_o == row_o // group) & (x == 0)
    cached = jnp.where(live_c, cached, FLOOR)
    own = jnp.where(live_o, own, FLOOR)
    top = jnp.maximum(
        jnp.max(cached, axis=1, keepdims=True), jnp.max(own, axis=1, keepdims=True)
    )
    w_c = jnp.where(live_c, jnp.exp(cached - top), 0.0)
    w_o = jnp.where(live_o, jnp.exp(own - top), 0.0)
    total = jnp.sum(w_c, axis=1, keepdims=True) + jnp.sum(w_o, axis=1, keepdims=True)
    z_bytes(3, vb).wait_recv()
    values = vb[...].reshape(NZ * span, HD)

    def weighted(w, v):
        high = w.astype(BF16)
        rest = (w - high.astype(F32)).astype(BF16)
        return jnp.dot(high, v, preferred_element_type=F32) + jnp.dot(
            rest, v, preferred_element_type=F32
        )

    mixed = weighted(w_c, values) + weighted(w_o, vx[...])
    lane_h = iota((n_heads, 128), 1)
    stats = jnp.where(lane_h < 64, top, total)
    for p in range(NX):
        ps[p] = jnp.concatenate([mixed[4 * p : 4 * p + 4], stats[4 * p : 4 * p + 4]], axis=0)
    pr[x] = ps[x]
    x_send(7, lambda p: ps.at[p], pr)
    x_bytes(7, pr).wait_recv()
    parts = [pr[p] for p in range(NX)]
    lane4 = iota((4, 128), 1)
    tops, sums = [], []
    for part in parts:
        st = part[4:8]
        turned = pltpu.roll(st, 64, axis=1)
        tops.append(jnp.where(lane4 < 64, st, turned))
        sums.append(jnp.where(lane4 < 64, turned, st))
    highest = tops[0]
    for t in tops[1:]:
        highest = jnp.maximum(highest, t)
    numerator = jnp.zeros((4, 128), F32)
    denominator = jnp.zeros((4, 128), F32)
    for part, t, l in zip(parts, tops, sums):
        scale = jnp.exp(t - highest)
        numerator = numerator + part[0:4] * scale
        denominator = denominator + l * scale
    attended = (numerator / denominator).astype(BF16)
    ats[...] = attended
    atr[z] = attended
    z_send(8, lambda p: ats, atr)
    for c in got_later:
        c.wait()
    z_bytes(8, atr).wait_recv()
    rows4 = [atr[b].astype(F32) for b in range(seqs)]
    for h in range(4):
        axs[:, 128 * h : 128 * h + 128] = jnp.concatenate(
            [r[h : h + 1] for r in rows4], axis=0
        ).astype(BF16)
    x_send(9, lambda p: axs, axr, xr_att)

    def columns(p):
        return pl.ds(pl.multiple_of(p * block, block), block)

    out_part = nt_dot(axs[...], wo_v[:, columns(x)])
    for o in X_ARRIVAL:
        p = x_peer(o)
        x_wait_one(9, axr, xr_att, p)
        out_part = out_part + nt_dot(axr[p], wo_v[:, columns(p)])
    out_part = widened(out_part)
    mos[...] = out_part
    swap = remote(mos, mor, 10, partner)
    swap.start()
    swap.wait_recv()
    both = out_part + mor[...]
    width = hid_v.shape[1]
    both = jnp.where(s == 0, both, pltpu.roll(both, 128 - width, axis=1))
    middle = (residual + both[:, :width]).astype(BF16).astype(F32)

    first = packed(middle).astype(BF16)
    mzs[...] = first
    mzr[z] = first
    z_send(11, lambda p: mzs, mzr)
    z_bytes(11, mzr).wait_recv()
    unpack_rows(mzr, mxs)
    x_send(12, lambda p: mxs, mxr, xr_mid)
    units = wg_v.shape[0]
    gate = jnp.zeros((seqs, units), F32)
    up = jnp.zeros((seqs, units), F32)
    squares = jnp.zeros((seqs, 128), F32)
    for o in [0] + X_ARRIVAL:
        p = x_peer(o)
        if o:
            x_wait_one(12, mxr, xr_mid, p)
            piece = mxr[p].astype(F32)
        else:
            piece = mxs[...].astype(F32)
        squares = squares + fold(piece)
        scaled = (piece * gf_v[:, columns(p)]).astype(BF16)
        gate = gate + nt_dot(scaled, wg_v[:, columns(p)])
        up = up + nt_dot(scaled, wu_v[:, columns(p)])
    ges[0] = widened(gate)
    ges[1] = widened(up)
    ges[2] = squares
    swap2 = remote(ges, ger, 13, partner)
    swap2.start()
    swap2.wait_recv()
    squares = jnp.sum(squares + ger[2], axis=1, keepdims=True)
    factor = lax.rsqrt(squares / (2 * half) + EPS)
    gate = (gate + ger[0][:, :units]) * factor
    up = (up + ger[1][:, :units]) * factor
    hidden = (gate / (1.0 + jnp.exp(-gate)) * up).astype(BF16)
    for o in X_ORDER + [0]:
        p = x_peer(o)
        piece = jnp.dot(hidden, wd_v[:, columns(p)], preferred_element_type=F32).astype(BF16)
        if o:
            dxs[p] = piece
            remote(dxs.at[p], dxr.at[x], 14, at(p, z)).start()
        else:
            dxr[p] = piece
    x_bytes(14, dxr).wait_recv()
    total = dxr[0].astype(F32)
    for p in range(1, NX):
        total = total + dxr[p].astype(F32)
    for m in range(NZ // 4):
        tile = block_transpose(total[:, 128 * m : 128 * m + 128])
        for i in range(4):
            dzs[4 * m + i] = tile[4 * i : 4 * i + 4].astype(BF16)
    dzr[z] = dzs[z]
    z_send(15, lambda p: dzs.at[p], dzr)
    z_bytes(15, dzr).wait_recv()
    total = dzr[0].astype(F32)
    for p in range(1, NZ):
        total = total + dzr[p].astype(F32)
    total = jnp.concatenate([total, jnp.zeros((12, 128), F32)], axis=0)
    down = block_transpose(total)[:, :width]
    out[...] = (middle + down).astype(BF16)

    def wait_sent(c, carry):
        chunk(r, h1s, partner).wait_send()
        return carry

    n_sent = r + jnp.where(r < NZ - 1, 1, 0) + jnp.where(r < NZ - 2, r + 1, 0)
    lax.fori_loop(0, n_sent, wait_sent, 0)
    x_bytes(1, xall.at[s]).wait_send()
    z_bytes(2, kb).wait_send()
    z_bytes(3, vb).wait_send()
    remote(xall.at[s], xall.at[s], 4, partner).wait_send()
    z_bytes(5, qr).wait_send()
    x_bytes(6, qxr).wait_send()
    x_bytes(7, pr).wait_send()
    z_bytes(8, atr).wait_send()
    x_bytes(9, axr).wait_send()
    swap.wait_send()
    z_bytes(11, mzr).wait_send()
    x_bytes(12, mxr).wait_send()
    swap2.wait_send()
    x_bytes(14, dxr).wait_send()
    z_bytes(15, dzr).wait_send()


def per_device(
    hidden_in, norm_attn, w_query, w_key, w_value, w_out, norm_ffn,
    w_gate, w_up, w_down, cache_keys, cache_values, lengths,
):
    seqs, _, width = hidden_in.shape
    model = w_query.shape[0]
    half = w_gate.shape[1]
    block = half // NX
    units = w_gate.shape[2]
    rows_q, rows_k = w_query.shape[2], w_key.shape[2]
    span, nk = cache_keys.shape[1], cache_keys.shape[2]
    freq = ROPE_BASE ** (-(np.arange(HD // 2, dtype=np.float64) * 2.0) / HD)
    freq = jnp.asarray(np.concatenate([freq, freq])[None].astype(np.float32))
    operands = (
        hidden_in.reshape(seqs, width),
        norm_attn.reshape(1, model),
        w_query.reshape(model, rows_q).T,
        w_key.reshape(model, rows_k).T,
        w_value.reshape(model, rows_k).T,
        w_out.reshape(half, -1).T,
        norm_ffn.reshape(1, model),
        w_gate.reshape(half, units).T,
        w_up.reshape(half, units).T,
        w_down.reshape(units, half),
        cache_keys.reshape(seqs, span * nk, HD),
        cache_values.reshape(seqs, span * nk, HD),
        lengths.reshape(1, seqs),
        freq,
    )
    vm = pltpu.VMEM
    scratch = [
        vm((seqs, width), BF16),
        vm((1, model), F32),
        vm((1, half), F32),
        vm((rows_q + 16, model), BF16),
        vm((rows_k, model), BF16),
        vm((rows_k, model), BF16),
        vm((operands[5].shape[0], half), BF16),
        vm((units, half), BF16),
        vm((units, half), BF16),
        vm((units, half), BF16),
        vm((NZ, span * nk, HD), BF16),
        vm((NZ, span * nk, HD), BF16),
        vm((16, HD), BF16),
        vm((16, HD), BF16),
        vm((1, seqs), jnp.int32),
        vm((1, 128), F32),
        vm((4, 128), BF16),
        vm((NZ, 4, 128), BF16),
        vm((2, NX, seqs, block), BF16),
        vm((seqs, 2, 128), F32),
        vm((NZ, 2, 128), F32),
        vm((8, 128), BF16),
        vm((NX, 8, 128), BF16),
        vm((NX, 8, 128), F32),
        vm((NX, 8, 128), F32),
        vm((4, 128), BF16),
        vm((NZ, 4, 128), BF16),
        vm((seqs, block), BF16),
        vm((NX, seqs, block), BF16),
        vm((seqs, 128), F32),
        vm((seqs, 128), F32),
        vm((4, 128), BF16),
        vm((NZ, 4, 128), BF16),
        vm((seqs, block), BF16),
        vm((NX, seqs, block), BF16),
        vm((3, seqs, 128), F32),
        vm((3, seqs, 128), F32),
        vm((NX, seqs, block), BF16),
        vm((NX, seqs, block), BF16),
        vm((NZ, 4, 128), BF16),
        vm((NZ, 4, 128), BF16),
        pltpu.SemaphoreType.DMA((14,)),
        pltpu.SemaphoreType.DMA((16,)),
        pltpu.SemaphoreType.DMA((16,)),
        pltpu.SemaphoreType.REGULAR((NZ,)),
        pltpu.SemaphoreType.REGULAR,
        pltpu.SemaphoreType.REGULAR,
        pltpu.SemaphoreType.REGULAR((NZ,)),
        pltpu.SemaphoreType.DMA((NZ,)),
        pltpu.SemaphoreType.DMA((NX,)),
        pltpu.SemaphoreType.DMA((NX,)),
        pltpu.SemaphoreType.DMA((NX,)),
        pltpu.SemaphoreType.DMA((NX,)),
        pltpu.SemaphoreType.DMA((NX,)),
    ]
    result = pl.pallas_call(
        kernel,
        out_shape=jax.ShapeDtypeStruct((seqs, width), BF16),
        in_specs=[pl.BlockSpec(memory_space=pl.ANY)] * len(operands),
        out_specs=pl.BlockSpec(memory_space=pltpu.VMEM),
        scratch_shapes=scratch,
        compiler_params=pltpu.CompilerParams(
            collective_id=0, has_side_effects=True, vmem_limit_bytes=60 * 1024 * 1024
        ),
    )(*operands)
    return result.reshape(seqs, 1, width)


def solution(mesh):
    return jax.shard_map(
        per_device,
        mesh=mesh,
        in_specs=(
            P("grp", "sub", "tp"),
            P(),
            P(None, "sub", "tp"),
            P(None, "sub", "tp"),
            P(None, "sub", "tp"),
            P("sub", None, None, "tp"),
            P(),
            P("sub", None, "tp"),
            P("sub", None, "tp"),
            P("tp", "sub", None),
            P("grp", "tp", "sub", None),
            P("grp", "tp", "sub", None),
            P("grp"),
        ),
        out_specs=P("grp", "sub", "tp"),
        check_vma=False,
    )
```
